32 devices in a mesh: row: 4 (over z), col: 8 (over y, x, core).
Axes of the slice: x: 2, y: 2, z: 4, core: 2. Of those that a mesh axis runs over, the one named last changes fastest.
Arguments:
- features: bfloat16 [32768, 256], P(('row', 'col')), may hold values from -6 to 6
- tile_values: bfloat16 [4, 8, 256, 128, 128], P('row', 'col'), may hold values from -0.09375 to 0.09375
- tile_rows: int32 [4, 8, 256], P('row', 'col'), may hold values from 0 to 63, as said below
- tile_cols: int32 [4, 8, 256], P('row', 'col'), may hold values from 0 to 31, as said below
- tile_count: int32 [4, 8], P('row', 'col'), may hold values from 64 to 256, as said below
- w_first: bfloat16 [256, 256], replicated, may hold values from -0.375 to 0.375
- w_second: bfloat16 [256, 256], replicated, may hold values from -0.375 to 0.375
Outputs:
- output: bfloat16 [32768, 256], P(('row', 'col'))
The draws below stay inside these ranges and needn't reach their ends.
Inputs may be any that keep to these rules, and one draw needn't show every extreme that they name: `tile_rows`: in each block the slots name distinct tiles; the first tile_count slots are ordered by tile column, then tile row; later slots are padding. `tile_cols`: as for tile_rows. `tile_count`: some block uses all 256 slots.
All inputs are finite; a program needn't handle non-finite values.
Results may differ from the reference program's by a relative error of at most 0.024.
Values may be sent and summed in bfloat16 or wider, within the bound.
No kernel may reach another device: no remote copies, remote signals or barrier semaphores. Data moves between devices by JAX's collectives and lax.ppermute only.
A program may use at most 192 MiB of HBM per device.

```python
import jax
import jax.numpy as jnp
from jax import lax

F = 256
TILE = 128
NODE_DEV = 1024
TILES = 256
TILE_ROWS = 64
TILE_COLS = 32
NODES = 32768
N_ROW = 4
N_COL = 8


def tile_layout(key):
    device_total = N_ROW * N_COL
    slots_total = TILE_ROWS * TILE_COLS
    layout_key = jax.random.fold_in(key, 4242)
    heaviest = jax.random.randint(jax.random.fold_in(layout_key, 1), (), 0, device_total)
    others = jax.random.randint(jax.random.fold_in(layout_key, 2), (device_total,), TILES // 4, TILES + 1)
    counts = jnp.where(jnp.arange(device_total, dtype=jnp.int32) == heaviest, TILES, others).astype(jnp.int32)

    def one_block(device, filled):
        chosen = jax.random.permutation(jax.random.fold_in(layout_key, 100 + device), slots_total)[:TILES]
        slot_ids = jnp.arange(TILES, dtype=jnp.int32)
        marked = jnp.where(slot_ids < filled, chosen, chosen + slots_total).astype(jnp.int32)
        ordered = jnp.sort(marked)
        flat_index = ordered % slots_total
        return (flat_index % TILE_ROWS, flat_index // TILE_ROWS)
    row_ids, col_ids = jax.vmap(one_block)(jnp.arange(device_total, dtype=jnp.int32), counts)
    return (row_ids.reshape(N_ROW, N_COL, TILES).astype(jnp.int32), col_ids.reshape(N_ROW, N_COL, TILES).astype(jnp.int32), counts.reshape(N_ROW, N_COL))


def draw_tile_rows(key, part):
    return tile_layout(key)[0]


def draw_tile_cols(key, part):
    return tile_layout(key)[1]


def draw_tile_count(key, part):
    return tile_layout(key)[2]


def block_levels(rng, shape, pieces, least, largest):
    def one(axis_at, parts):
        draws = jax.random.uniform(jax.random.fold_in(jax.random.fold_in(rng, 6), axis_at), (parts,), jnp.float32, least / len(pieces), largest / len(pieces))
        return jnp.repeat(jnp.exp(draws), shape[axis_at] // parts).reshape((-1,) + (1,) * (len(shape) - axis_at - 1))

    factor_of = one(*pieces[0])
    for cut in pieces[1:]:
        factor_of = factor_of * one(*cut)
    return factor_of


def centred(own_key, extent, width, most, cuts=(), held_as=jnp.bfloat16):
    drawn = jax.random.normal(own_key, extent, jnp.float32) * width
    if len(cuts) > 0:
        drawn = block_levels(own_key, extent, cuts, -0.22, 0.18) * drawn
    return jnp.clip(drawn, min=-most, max=most).astype(held_as)


def setup_inputs(seed: int = 0) -> dict:
    key_of = jax.random.split(jax.random.key(seed), 8)
    return {
        "features": centred(key_of[0], (NODES, F), 1.0, 6.0, ((0, 32),)),
        "tile_values": centred(key_of[1], (N_ROW, N_COL, TILES, TILE, TILE), (TILES * TILE * TILE // NODE_DEV) ** -0.5, 0.09375, ((0, 4), (1, 8))),
        "tile_rows": draw_tile_rows(jax.random.fold_in(key_of[7], 71), 0),
        "tile_cols": draw_tile_cols(jax.random.fold_in(key_of[7], 71), 0),
        "tile_count": draw_tile_count(jax.random.fold_in(key_of[7], 71), 0),
        "w_first": centred(key_of[5], (F, F), F ** -0.5, 0.375),
        "w_second": centred(key_of[6], (F, F), F ** -0.5, 0.375),
    }


def block_partial(values, row_ids, col_ids, filled, panel_tiles):
    active = (jnp.arange(TILES, dtype=jnp.int32) < filled).astype(jnp.float32)
    inputs = panel_tiles[col_ids].astype(jnp.float32)
    products = jnp.einsum("gij,gjf->gif", values.astype(jnp.float32), inputs) * active[:, None, None]
    return jax.ops.segment_sum(products, row_ids, num_segments=TILE_ROWS)


def aggregate(inputs_now, tile_values, tile_rows, tile_cols, tile_count):
    blocks = inputs_now.reshape(N_ROW, N_COL, NODE_DEV, F)

    def row_block(row_index):
        def add_col(running, col_index):
            panel_tiles = blocks[:, col_index].reshape(N_ROW * NODE_DEV // TILE, TILE, F)
            partial_value = block_partial(tile_values[row_index, col_index], tile_rows[row_index, col_index],
                                    tile_cols[row_index, col_index], tile_count[row_index, col_index], panel_tiles)
            rounded = lax.optimization_barrier(partial_value.astype(jnp.bfloat16))
            return running + rounded.astype(jnp.float32), None

        running, unused = lax.scan(add_col, jnp.zeros((TILE_ROWS, TILE, F), jnp.float32),
                                   jnp.arange(N_COL, dtype=jnp.int32))
        return running.astype(jnp.bfloat16)

    summed = lax.map(row_block, jnp.arange(N_ROW, dtype=jnp.int32))
    return summed.reshape(N_ROW * N_COL * NODE_DEV, F)


def reference(features, tile_values, tile_rows, tile_cols, tile_count, w_first, w_second):
    summed = aggregate(features, tile_values, tile_rows, tile_cols, tile_count)
    hidden = jax.nn.relu(jnp.dot(summed, w_first, preferred_element_type=jnp.float32)).astype(jnp.bfloat16)
    summed_two = aggregate(hidden, tile_values, tile_rows, tile_cols, tile_count)
    return jax.nn.relu(jnp.dot(summed_two, w_second, preferred_element_type=jnp.float32)).astype(jnp.bfloat16)
```

```python
import functools

import jax
import jax.numpy as jnp
from jax import lax
from jax.experimental import pallas as pl
from jax.experimental.pallas import tpu as pltpu
from jax.sharding import PartitionSpec as P

CHUNKS = 2
GROUP = 8


def spmm_kernel(rows, cols, span, values, panels, outs, acc, tiles, sems):
    count = len(panels)
    tile = tiles.shape[-1]
    slots = values.shape[0]
    width = acc.shape[1]
    spare = acc.shape[0] // tile - 1
    lo, hi = span[0], span[1]
    groups = (hi + GROUP - 1) // GROUP - lo // GROUP
    first = lo // GROUP

    def fetch(i):
        return pltpu.make_async_copy(
            values.at[pl.ds((first + i) * GROUP, GROUP)], tiles.at[pl.ds(i * GROUP, GROUP)], sems.at[i]
        )

    @pl.loop(0, groups)
    def _(i):
        fetch(i).start()

    @pl.loop(0, acc.shape[0] // tile)
    def _(i):
        acc[pl.ds(i * tile, tile), :] = jnp.zeros((tile, width), jnp.float32)

    per = panels[0].shape[0] // tile

    @pl.loop(0, groups)
    def _(i):
        fetch(i).wait()
        products = []
        targets = []
        for g in range(GROUP):
            slot = (first + i) * GROUP + g
            live = (slot >= lo) & (slot < hi)
            col = jnp.where(live, cols[slot], 0)
            targets.append(jnp.where(live, rows[slot], spare))
            products.append(
                jnp.dot(
                    tiles[i * GROUP + g],
                    panels[0][pl.ds(col * tile, tile), :],
                    preferred_element_type=jnp.float32,
                )
            )
        for g in range(GROUP):
            at = pl.ds(targets[g] * tile, tile)
            acc[at, :] += products[g]

    base = 0
    for out in outs:
        n = out.shape[0]

        @pl.loop(0, n // tile)
        def _(i):
            out[pl.ds(i * tile, tile), :] = acc[pl.ds(base + i * tile, tile), :].astype(out.dtype)

        base += n


def spmm(rows, cols, span, values, panel, row_tiles):
    slots, tile, _ = values.shape
    width = panel.shape[1]
    half = row_tiles // 2 * tile
    smem = pl.BlockSpec(memory_space=pltpu.SMEM)
    vmem = pl.BlockSpec(memory_space=pltpu.VMEM)

    def body(rows, cols, span, values, panel, keep, send, acc, tiles, sems):
        spmm_kernel(rows, cols, span, values, [panel], [keep, send], acc, tiles, sems)

    shape = jax.ShapeDtypeStruct((half, width), jnp.bfloat16)
    return pl.pallas_call(
        body,
        out_shape=(shape, shape),
        in_specs=[smem, smem, smem, pl.BlockSpec(memory_space=pl.ANY), vmem],
        out_specs=(vmem, vmem),
        scratch_shapes=[
            pltpu.VMEM(((row_tiles + 1) * tile, width), jnp.float32),
            pltpu.VMEM((slots, tile, tile), jnp.bfloat16),
            pltpu.SemaphoreType.DMA((slots // GROUP,)),
        ],
        compiler_params=pltpu.CompilerParams(vmem_limit_bytes=40 * 1024 * 1024),
        cost_estimate=pl.CostEstimate(
            flops=2 * slots * tile * tile * width, bytes_accessed=values.size * 2, transcendentals=0
        ),
        name="spmm",
    )(rows, cols, span, values, panel)


def shift(n, step):
    return [(i, i + step) for i in range(n) if 0 <= i + step < n]


def gather_line(block, n):
    me = lax.axis_index("row")
    panel = jnp.zeros((n,) + block.shape, block.dtype)
    panel = lax.dynamic_update_index_in_dim(panel, block, me, 0)
    up = down = block
    for r in range(1, n):
        up = lax.ppermute(up, "row", shift(n, 1))
        down = lax.ppermute(down, "row", shift(n, -1))
        lower = jnp.maximum(me - r, 0)
        upper = jnp.minimum(me + r, n - 1)
        old = lax.dynamic_index_in_dim(panel, lower, 0, keepdims=False)
        panel = lax.dynamic_update_index_in_dim(panel, jnp.where(me - r >= 0, up, old), lower, 0)
        old = lax.dynamic_index_in_dim(panel, upper, 0, keepdims=False)
        panel = lax.dynamic_update_index_in_dim(panel, jnp.where(me + r < n, down, old), upper, 0)
    return panel.reshape(-1, block.shape[1])


def reduce_blocks(keep, send, n, size):
    got = lax.ppermute(send, "col", [(i, i ^ 1) for i in range(n)])
    both = []
    for j in range(n // 2):
        at = slice(j * size, (j + 1) * size)
        both.append((keep[at].astype(jnp.float32) + got[at].astype(jnp.float32)).astype(jnp.bfloat16))
    arrived = [both[0]]
    for j in range(1, n // 2):
        arrived.append(lax.ppermute(both[j], "col", [(i, i ^ (2 * j)) for i in range(n)]))
    total = arrived[0].astype(jnp.float32)
    for one in arrived[1:]:
        total = total + one.astype(jnp.float32)
    return total.astype(jnp.bfloat16)


def layer(pieces, weight, tables, values, n_row, n_col):
    rows, cols, span, row_tiles = tables
    width = pieces[0].shape[1]
    total = None
    for k, piece in enumerate(pieces):
        panel = gather_line(piece, n_row)
        keep, send = spmm(rows, cols, span, values, panel, row_tiles)
        summed = reduce_blocks(keep, send, n_col, piece.shape[0])
        term = jnp.dot(
            summed, weight[k * width : (k + 1) * width], preferred_element_type=jnp.float32
        )
        total = term if total is None else total + term
    return jax.nn.relu(total).astype(jnp.bfloat16)


def shards(n_row, n_col, features, tile_values, tile_rows, tile_cols, tile_count, w_first, w_second):
    values = tile_values[0, 0]
    row_ids = tile_rows[0, 0]
    col_ids = tile_cols[0, 0]
    filled = tile_count[0, 0]
    tile = values.shape[-1]
    node_dev, feature_width = features.shape
    per = node_dev // tile
    row_tiles = per * n_col
    me = lax.axis_index("col")
    relative = (row_ids // per) ^ me
    rows = ((relative & 1) * (n_col // 2) + (relative >> 1)) * per + row_ids % per
    span = jnp.stack([jnp.zeros_like(filled), filled])
    tables = (rows, col_ids, span, row_tiles)
    width = feature_width // CHUNKS

    def cut(x):
        return [x[:, k * width : (k + 1) * width] for k in range(CHUNKS)]

    hidden = layer(cut(features), w_first, tables, values, n_row, n_col)
    return layer(cut(hidden), w_second, tables, values, n_row, n_col)


def solution(mesh):
    n_row, n_col = mesh.shape["row"], mesh.shape["col"]
    return jax.shard_map(
        functools.partial(shards, n_row, n_col),
        mesh=mesh,
        in_specs=(
            P(("row", "col"), None),
            P("row", "col", None, None, None),
            P("row", "col", None),
            P("row", "col", None),
            P("row", "col"),
            P(),
            P(),
        ),
        out_specs=P(("row", "col"), None),
        check_vma=False,
    )
```
